32 devices in a mesh: pod: 1 (over z), dp: 4 (over y), tp: 8 (over x, core).
Axes of the slice: x: 4, y: 4, z: 1, core: 2. Of those that a mesh axis runs over, the one named last changes fastest.
The devices are a block of a 4x4x8 slice.
Arguments:
- x_saved: bfloat16 [6144, 2048], P(('pod', 'dp'))
- h_saved: bfloat16 [6144, 2048], P(('pod', 'dp'))
- mean_one: float32 [6144], P(('pod', 'dp'))
- rstd_one: float32 [6144], P(('pod', 'dp'))
- mean_two: float32 [6144], P(('pod', 'dp'))
- rstd_two: float32 [6144], P(('pod', 'dp'))
- gain_one: bfloat16 [2048], replicated
- gain_two: bfloat16 [2048], replicated
- grad_y: bfloat16 [6144, 2048], P(('pod', 'dp'))
- w_qkv: bfloat16 [2048, 3, 32, 64], P(None, None, 'tp')
- w_proj: bfloat16 [32, 64, 2048], P('tp')
- w_up: bfloat16 [2048, 8192], P(None, 'tp')
- w_down: bfloat16 [8192, 2048], P('tp')
Outputs:
- output 1: bfloat16 [6144, 2048], P(('pod', 'dp'))
- output 2: bfloat16 [2048, 3, 32, 64], P('pod', None, 'tp')
- output 3: bfloat16 [32, 64, 2048], P(('pod', 'tp'))
- output 4: bfloat16 [2048, 8192], P('pod', 'tp')
- output 5: bfloat16 [8192, 2048], P(('pod', 'tp'))
All inputs are finite; a program needn't handle non-finite values.
Results may differ from the reference program's by a relative error of at most 0.0192615.
Values are sent between devices in bfloat16 or wider.
A program may use at most 768 MiB of HBM per device.

```python
import math
import jax
import jax.numpy as jnp
from jax import lax

MODEL_DIM = 2048
NUM_HEADS = 32
FFN_DIM = 8192
TOKENS = 1536
DATA_WAYS = 4

HEAD_DIM = MODEL_DIM // NUM_HEADS
ROW_COUNT = DATA_WAYS * TOKENS
QK_GAIN = (2.0 * math.log(TOKENS)) ** 0.25
GELU_C = math.sqrt(2.0 / math.pi)


def saved_stats(rows_wide):
    row_mean = jnp.mean(rows_wide, axis=-1)
    row_var = jnp.mean(jnp.square(rows_wide - row_mean[:, None]), axis=-1)
    return row_mean, 1.0 / jnp.sqrt(row_var + 1e-5)


def setup_inputs(seed: int = 0, part: int = 0) -> dict:
    shared_keys = jax.random.split(jax.random.key(seed), 6)
    own_keys = jax.random.split(jax.random.fold_in(jax.random.key(seed + 1), part), 7)
    x_rows = jnp.exp(jax.random.uniform(own_keys[3], (ROW_COUNT, 1), jnp.float32, -0.7, 0.7))
    h_rows = jnp.exp(jax.random.uniform(own_keys[4], (ROW_COUNT, 1), jnp.float32, -0.7, 0.7))
    x_shift = 0.5 * jax.random.normal(own_keys[5], (ROW_COUNT, 1), jnp.float32)
    h_shift = 0.5 * jax.random.normal(own_keys[6], (ROW_COUNT, 1), jnp.float32)
    x_saved = (jax.random.normal(own_keys[0], (ROW_COUNT, MODEL_DIM), jnp.float32) * x_rows + x_shift).astype(jnp.bfloat16)
    h_saved = (jax.random.normal(own_keys[1], (ROW_COUNT, MODEL_DIM), jnp.float32) * h_rows + h_shift).astype(jnp.bfloat16)
    grad_y = jax.random.normal(own_keys[2], (ROW_COUNT, MODEL_DIM), jnp.float32).astype(jnp.bfloat16)
    mean_one, rstd_one = saved_stats(x_saved.astype(jnp.float32))
    mean_two, rstd_two = saved_stats(h_saved.astype(jnp.float32))
    gain_one = (1.0 + 0.3 * jax.random.normal(shared_keys[0], (MODEL_DIM,), jnp.float32)).astype(jnp.bfloat16)
    gain_two = (1.0 + 0.3 * jax.random.normal(shared_keys[1], (MODEL_DIM,), jnp.float32)).astype(jnp.bfloat16)
    qkv_scale = jnp.array([QK_GAIN, QK_GAIN, 1.0], jnp.float32)[None, :, None, None] * MODEL_DIM ** -0.5
    w_qkv = (jax.random.normal(shared_keys[2], (MODEL_DIM, 3, NUM_HEADS, HEAD_DIM), jnp.float32) * qkv_scale).astype(jnp.bfloat16)
    w_proj = (jax.random.normal(shared_keys[3], (NUM_HEADS, HEAD_DIM, MODEL_DIM), jnp.float32) * MODEL_DIM ** -0.5).astype(jnp.bfloat16)
    w_up = (jax.random.normal(shared_keys[4], (MODEL_DIM, FFN_DIM), jnp.float32) * MODEL_DIM ** -0.5).astype(jnp.bfloat16)
    w_down = (jax.random.normal(shared_keys[5], (FFN_DIM, MODEL_DIM), jnp.float32) * FFN_DIM ** -0.5).astype(jnp.bfloat16)
    return {'x_saved': x_saved, 'h_saved': h_saved, 'mean_one': mean_one, 'rstd_one': rstd_one,
            'mean_two': mean_two, 'rstd_two': rstd_two, 'gain_one': gain_one, 'gain_two': gain_two,
            'grad_y': grad_y, 'w_qkv': w_qkv, 'w_proj': w_proj, 'w_up': w_up, 'w_down': w_down}


def layer_norm(row_vals, row_mean, row_rstd, gain_vec):
    x_hat = (row_vals.astype(jnp.float32) - row_mean[:, None]) * row_rstd[:, None]
    return x_hat, (x_hat * gain_vec.astype(jnp.float32)).astype(jnp.bfloat16)


def norm_back(d_norm, x_hat, row_rstd, gain_vec):
    scaled = d_norm * gain_vec.astype(jnp.float32)
    scaled_mean = jnp.mean(scaled, axis=-1, keepdims=True)
    proj_mean = jnp.mean(scaled * x_hat, axis=-1, keepdims=True)
    return row_rstd[:, None] * (scaled - scaled_mean - x_hat * proj_mean)


def gelu_pair(pre_act):
    pre_wide = pre_act.astype(jnp.float32)
    tanh_val = jnp.tanh(GELU_C * (pre_wide + 0.044715 * pre_wide * pre_wide * pre_wide))
    gelu_val = 0.5 * pre_wide * (1.0 + tanh_val)
    gelu_slope = 0.5 * (1.0 + tanh_val) + 0.5 * pre_wide * (1.0 - tanh_val * tanh_val) * GELU_C * (1.0 + 0.134145 * pre_wide * pre_wide)
    return gelu_val, gelu_slope


def head_pass(head_in):
    qkv_head, dout_head = head_in
    q_head = qkv_head[:, 0]
    k_head = qkv_head[:, 1]
    v_head = qkv_head[:, 2]
    scores = jnp.dot(q_head, k_head.T, preferred_element_type=jnp.float32) * HEAD_DIM ** -0.5
    row_ids = lax.broadcasted_iota(jnp.int32, (TOKENS, TOKENS), 0)
    col_ids = lax.broadcasted_iota(jnp.int32, (TOKENS, TOKENS), 1)
    scores = jnp.where(col_ids <= row_ids, scores, -1e30)
    shifted = jnp.exp(scores - jnp.max(scores, axis=-1, keepdims=True))
    prob_mat = shifted / jnp.sum(shifted, axis=-1, keepdims=True)
    prob_lo = prob_mat.astype(jnp.bfloat16)
    head_out = jnp.dot(prob_lo, v_head, preferred_element_type=jnp.float32).astype(jnp.bfloat16)
    dv_head = jnp.dot(prob_lo.T, dout_head, preferred_element_type=jnp.float32).astype(jnp.bfloat16)
    d_probs = jnp.dot(dout_head, v_head.T, preferred_element_type=jnp.float32)
    d_scores = (prob_mat * (d_probs - jnp.sum(prob_mat * d_probs, axis=-1, keepdims=True)) * HEAD_DIM ** -0.5).astype(jnp.bfloat16)
    dq_head = jnp.dot(d_scores, k_head, preferred_element_type=jnp.float32).astype(jnp.bfloat16)
    dk_head = jnp.dot(d_scores.T, q_head, preferred_element_type=jnp.float32).astype(jnp.bfloat16)
    return head_out, jnp.stack([dq_head, dk_head, dv_head], axis=1)


def reference(x_saved, h_saved, mean_one, rstd_one, mean_two, rstd_two, gain_one, gain_two, grad_y, w_qkv, w_proj, w_up, w_down):
    qkv_wide = w_qkv.astype(jnp.float32)
    proj_wide = w_proj.astype(jnp.float32)

    def seq_pass(carry, seq_in):
        acc_qkv, acc_proj, acc_up, acc_down = carry
        x_seq, h_seq, mean_a, rstd_a, mean_b, rstd_b, dy_seq = seq_in
        hat_two, norm_two = layer_norm(h_seq, mean_b, rstd_b, gain_two)
        pre_act = jnp.dot(norm_two, w_up, preferred_element_type=jnp.float32).astype(jnp.bfloat16)
        gelu_val, gelu_slope = gelu_pair(pre_act)
        act_out = gelu_val.astype(jnp.bfloat16)
        d_pre = (jnp.dot(dy_seq, w_down.T, preferred_element_type=jnp.float32) * gelu_slope).astype(jnp.bfloat16)
        acc_up = acc_up + jnp.dot(norm_two.T, d_pre, preferred_element_type=jnp.float32)
        acc_down = acc_down + jnp.dot(act_out.T, dy_seq, preferred_element_type=jnp.float32)
        d_norm_two = jnp.dot(d_pre, w_up.T, preferred_element_type=jnp.float32)
        d_mid = dy_seq.astype(jnp.float32) + norm_back(d_norm_two, hat_two, rstd_b, gain_two)
        d_mid_lo = d_mid.astype(jnp.bfloat16)
        hat_one, norm_one = layer_norm(x_seq, mean_a, rstd_a, gain_one)
        qkv_heads = jnp.einsum('td,dche->tche', norm_one.astype(jnp.float32), qkv_wide).astype(jnp.bfloat16)
        d_attn = jnp.einsum('td,hed->the', d_mid_lo.astype(jnp.float32), proj_wide).astype(jnp.bfloat16)
        head_outs, head_grads = lax.map(head_pass, (jnp.moveaxis(qkv_heads, 2, 0), jnp.moveaxis(d_attn, 1, 0)))
        attn_out = jnp.moveaxis(head_outs, 0, 1)
        d_qkv = jnp.moveaxis(head_grads, 0, 2).astype(jnp.float32)
        acc_proj = acc_proj + jnp.einsum('the,td->hed', attn_out.astype(jnp.float32), d_mid_lo.astype(jnp.float32))
        acc_qkv = acc_qkv + jnp.einsum('td,tche->dche', norm_one.astype(jnp.float32), d_qkv)
        d_norm_one = jnp.einsum('tche,dche->td', d_qkv, qkv_wide)
        grad_x = (d_mid + norm_back(d_norm_one, hat_one, rstd_a, gain_one)).astype(jnp.bfloat16)
        return (acc_qkv, acc_proj, acc_up, acc_down), grad_x

    zero_sums = (jnp.zeros((MODEL_DIM, 3, NUM_HEADS, HEAD_DIM), jnp.float32),
                 jnp.zeros((NUM_HEADS, HEAD_DIM, MODEL_DIM), jnp.float32),
                 jnp.zeros((MODEL_DIM, FFN_DIM), jnp.float32),
                 jnp.zeros((FFN_DIM, MODEL_DIM), jnp.float32))
    seq_inputs = (x_saved.reshape(DATA_WAYS, TOKENS, MODEL_DIM), h_saved.reshape(DATA_WAYS, TOKENS, MODEL_DIM),
                  mean_one.reshape(DATA_WAYS, TOKENS), rstd_one.reshape(DATA_WAYS, TOKENS),
                  mean_two.reshape(DATA_WAYS, TOKENS), rstd_two.reshape(DATA_WAYS, TOKENS),
                  grad_y.reshape(DATA_WAYS, TOKENS, MODEL_DIM))
    grad_sums, grad_rows = lax.scan(seq_pass, zero_sums, seq_inputs)
    acc_qkv, acc_proj, acc_up, acc_down = grad_sums
    return (grad_rows.reshape(ROW_COUNT, MODEL_DIM), acc_qkv.astype(jnp.bfloat16), acc_proj.astype(jnp.bfloat16),
            acc_up.astype(jnp.bfloat16), acc_down.astype(jnp.bfloat16))
```

```python
import functools
import math
import jax
import jax.numpy as jnp
from jax import lax
from jax.experimental import pallas as pl
from jax.experimental.pallas import tpu as pltpu
from jax.sharding import PartitionSpec as P

GELU_C = math.sqrt(2.0 / math.pi)
LOG2E = math.log2(math.e)
NT = (((1,), (1,)), ((), ()))
NN = (((1,), (0,)), ((), ()))
TN = (((0,), (0,)), ((), ()))


def dot(lhs, rhs, dims=NN):
    return lax.dot_general(lhs, rhs, dims, preferred_element_type=jnp.float32)


def normed(row_vals, row_mean, row_rstd):
    return (row_vals.astype(jnp.float32) - row_mean[:, None]) * row_rstd[:, None]


def norm_back(d_norm, x_hat, row_rstd, gain_vec):
    scaled = d_norm * gain_vec.astype(jnp.float32)
    scaled_mean = jnp.mean(scaled, axis=-1, keepdims=True)
    proj_mean = jnp.mean(scaled * x_hat, axis=-1, keepdims=True)
    return row_rstd[:, None] * (scaled - scaled_mean - x_hat * proj_mean)


def gelu_pair(pre_act):
    pre_wide = pre_act.astype(jnp.float32)
    tanh_val = jnp.tanh(GELU_C * (pre_wide + 0.044715 * pre_wide * pre_wide * pre_wide))
    gelu_val = 0.5 * pre_wide * (1.0 + tanh_val)
    gelu_slope = 0.5 * (1.0 + tanh_val) + 0.5 * pre_wide * (1.0 - tanh_val * tanh_val) * GELU_C * (1.0 + 0.134145 * pre_wide * pre_wide)
    return gelu_val, gelu_slope


def attn_kernel(head_dim, q_rows, q_ref, k_ref, v_ref, do_ref, o_ref, dqkv_ref, dk_acc, dv_acc):
    toks, lanes = q_ref.shape
    step = pl.program_id(0)
    per_block = lanes // head_dim
    group = step // per_block
    inner = lax.rem(step, per_block)
    width = dqkv_ref.shape[1] // 3
    scale = head_dim ** -0.5

    @pl.when(inner == 0)
    def _():
        dk_acc[...] = jnp.zeros_like(dk_acc)
        dv_acc[...] = jnp.zeros_like(dv_acc)
        o_ref[...] = jnp.zeros_like(o_ref)
        dqkv_ref[:, pl.ds(pl.multiple_of(group * lanes, lanes), lanes)] = jnp.zeros((toks, lanes), dqkv_ref.dtype)

    lane_ids = lax.broadcasted_iota(jnp.int32, (1, lanes), 1)
    mine = lane_ids // head_dim == inner
    zero = jnp.zeros((), jnp.bfloat16)
    k_own = jnp.where(mine, k_ref[...], zero)
    v_own = jnp.where(mine, v_ref[...], zero)
    k_t = k_own.T
    v_t = v_own.T
    q_cols = pl.ds(pl.multiple_of(group * lanes, lanes), lanes)
    for blk in range(toks // q_rows):
        rows = slice(blk * q_rows, (blk + 1) * q_rows)
        keys = (blk + 1) * q_rows
        q_blk = jnp.where(mine, q_ref[rows, :], zero)
        do_blk = jnp.where(mine, do_ref[rows, :], zero)
        s_t = dot(k_own[:keys], q_blk, NT)
        key_ids = lax.broadcasted_iota(jnp.int32, (q_rows, q_rows), 0)
        qry_ids = lax.broadcasted_iota(jnp.int32, (q_rows, q_rows), 1)
        s_diag = jnp.where(key_ids <= qry_ids, s_t[keys - q_rows:], -1e30)
        s_t = s_diag if blk == 0 else jnp.concatenate([s_t[:keys - q_rows], s_diag], axis=0)
        top = jnp.max(s_t, axis=0, keepdims=True)
        e_t = jnp.exp2((s_t - top) * (scale * LOG2E))
        p_t = e_t * (1.0 / jnp.sum(e_t, axis=0, keepdims=True))
        p_lo = p_t.astype(jnp.bfloat16)
        dp_t = dot(v_own[:keys], do_blk, NT)
        dv_acc[:keys] += dot(p_lo, do_blk)
        o_blk = dot(v_t[:, :keys], p_lo)
        o_ref[rows, :] += o_blk.T.astype(o_ref.dtype)
        prod = p_t * dp_t
        row_sum = jnp.sum(prod, axis=0, keepdims=True)
        ds_lo = (prod - p_t * row_sum).astype(jnp.bfloat16)
        dk_acc[:keys] += dot(ds_lo, q_blk)
        dq_blk = dot(k_t[:, :keys], ds_lo) * scale
        dqkv_ref[rows, q_cols] += dq_blk.T.astype(dqkv_ref.dtype)

    @pl.when(inner == per_block - 1)
    def _():
        dqkv_ref[:, pl.ds(pl.multiple_of(width + group * lanes, lanes), lanes)] = (dk_acc[...] * scale).astype(dqkv_ref.dtype)
        dqkv_ref[:, pl.ds(pl.multiple_of(2 * width + group * lanes, lanes), lanes)] = dv_acc[...].astype(dqkv_ref.dtype)


def attention(qkv, d_attn, heads, head_dim, q_rows=256):
    toks, width = d_attn.shape
    lanes = 128
    per_block = lanes // head_dim
    groups = width // lanes
    spec = lambda off: pl.BlockSpec((toks, lanes), lambda h: (0, off * groups + h // per_block))
    pairs = heads * toks * toks // 2
    return pl.pallas_call(
        functools.partial(attn_kernel, head_dim, q_rows),
        grid=(heads,),
        in_specs=[spec(0), spec(1), spec(2), spec(0)],
        out_specs=[spec(0), pl.BlockSpec((toks, 3 * width), lambda h: (0, 0))],
        out_shape=[jax.ShapeDtypeStruct((toks, width), jnp.bfloat16), jax.ShapeDtypeStruct((toks, 3 * width), jnp.bfloat16)],
        scratch_shapes=[pltpu.VMEM((toks, lanes), jnp.float32), pltpu.VMEM((toks, lanes), jnp.float32)],
        compiler_params=pltpu.CompilerParams(dimension_semantics=("arbitrary",), vmem_limit_bytes=48 * 2 ** 20),
        cost_estimate=pl.CostEstimate(flops=6 * 2 * 256 * pairs, bytes_accessed=8 * toks * width * 2, transcendentals=pairs),
        name="attn_fwd_bwd",
    )(qkv, qkv, qkv, d_attn)


def after(first, *later):
    out = lax.optimization_barrier((first,) + later)[1:]
    return out[0] if len(out) == 1 else out


def wide(arr):
    return arr.astype(jnp.float32)


class Ring:
    def __init__(self, axis, ways, lanes):
        self.axis, self.n, self.lanes = axis, ways // lanes, lanes
        self.me = lax.axis_index(axis) // lanes
        hop = lambda d: [(i, ((i // lanes + d) % self.n) * lanes + i % lanes) for i in range(ways)]
        self.right, self.left = hop(1), hop(-1)

    def to(self, arr, pairs):
        return lax.ppermute(arr, self.axis, pairs)

    def at(self, d):
        return lax.rem(self.me + d + self.n, self.n)

    def gather(self, own):
        half = own.shape[0] // 2
        pieces = [(0, 0, own)]
        from_left = from_right = own
        for k in range(1, self.n // 2):
            from_left, from_right = self.to(from_left, self.right), self.to(from_right, self.left)
            pieces += [(-k, 0, from_left), (k, 0, from_right)]
        pieces += [(self.n // 2, 0, self.to(from_left[:half], self.right)), (self.n // 2, half, self.to(from_right[half:], self.left))]
        return pieces

    def placed(self, pieces, rows):
        out = jnp.zeros((self.n * rows,) + pieces[0][2].shape[1:], pieces[0][2].dtype)
        for offset, row, piece in pieces:
            out = lax.dynamic_update_slice_in_dim(out, piece, self.at(offset) * rows + row, 0)
        return out

    def scatter(self, blocks, filler):
        dtype = blocks.dtype
        half = blocks.shape[1] // 2
        blk = lambda d: lax.dynamic_index_in_dim(blocks, self.at(d), 0, keepdims=False)
        far = blk(self.n // 2)
        right, left = self.to(far[:half], self.right), self.to(far[half:], self.left)
        if filler is not None:
            right, left = after(filler, right, left)
        for k in range(self.n // 2 - 1, 0, -1):
            go_right, go_left = blk(k), blk(-k)
            if right.shape[0] == half:
                go_right = jnp.concatenate([(wide(go_right[:half]) + wide(right)).astype(dtype), go_right[half:]], 0)
                go_left = jnp.concatenate([go_left[:half], (wide(go_left[half:]) + wide(left)).astype(dtype)], 0)
            else:
                go_right = (wide(go_right) + wide(right)).astype(dtype)
                go_left = (wide(go_left) + wide(left)).astype(dtype)
            right, left = self.to(go_right, self.right), self.to(go_left, self.left)
        return wide(blk(0)) + wide(right) + wide(left)


def solution(mesh):
    row_spec = P(('pod', 'dp'), None)
    stat_spec = P(('pod', 'dp'))
    in_specs = (row_spec, row_spec, stat_spec, stat_spec, stat_spec, stat_spec, P(None), P(None), row_spec,
                P(None, None, 'tp', None), P('tp', None, None), P(None, 'tp'), P('tp', None))
    out_specs = (row_spec, P('pod', None, 'tp', None), P(('pod', 'tp'), None, None), P('pod', 'tp'), P(('pod', 'tp'), None))
    tp_ways, dp_ways = mesh.shape['tp'], mesh.shape['dp']
    cores = 2

    def local_step(x_saved, h_saved, mean_one, rstd_one, mean_two, rstd_two, gain_one, gain_two, grad_y, w_qkv, w_proj, w_up, w_down):
        toks, dim = x_saved.shape
        _, three, heads, head_dim = w_qkv.shape
        share = toks // tp_ways
        chips = tp_ways // cores
        tp_at = lax.axis_index('tp')
        start = tp_at * share
        cut = lambda arr: lax.dynamic_slice_in_dim(arr, start, share, 0)
        w_qkv_flat = w_qkv.reshape(dim, three * heads * head_dim)
        w_proj_flat = w_proj.reshape(heads * head_dim, dim)
        lo = jnp.bfloat16
        dp_ring = Ring('dp', dp_ways, 1)
        tp_ring = Ring('tp', tp_ways, cores)
        core = lax.rem(tp_at, cores)
        sibling = [(i, i ^ 1) for i in range(tp_ways)]

        def tp_scatter(part, first, second):
            by_core = part.reshape(chips, cores, share, dim)
            mine = lax.dynamic_index_in_dim(by_core, core, 1, keepdims=False)
            other = lax.dynamic_index_in_dim(by_core, 1 - core, 1, keepdims=False)
            other = after(first, lax.ppermute(other, 'tp', sibling))
            pair = (wide(mine) + wide(other)).astype(part.dtype)
            return tp_ring.scatter(pair, second)

        def tp_gather(own, out, first=None):
            for offset, row, piece in tp_ring.gather(own):
                if offset != 0 and first is not None:
                    piece = after(first, piece)
                base = tp_ring.at(offset) * cores
                other = lax.ppermute(piece, 'tp', sibling)
                out = lax.dynamic_update_slice_in_dim(out, piece, (base + core) * share + row, 0)
                out = lax.dynamic_update_slice_in_dim(out, other, (base + 1 - core) * share + row, 0)
            return out

        def dp_scatter(part):
            return lax.psum_scatter(part, 'dp', scatter_dimension=0, tiled=True)

        norm_two = (normed(h_saved, mean_two, rstd_two) * wide(gain_two)).astype(lo)
        pre_act = dot(norm_two, w_up).astype(lo)
        act_out = gelu_pair(pre_act)[0].astype(lo)
        part_down = dot(act_out, grad_y, TN)
        own_down = dp_scatter(part_down)
        pre_act, dy = after(part_down, pre_act, grad_y)
        d_pre = (dot(dy, w_down, NT) * gelu_pair(pre_act)[1]).astype(lo)
        part_two = dot(d_pre, w_up, NT).astype(lo)
        part_up = dot(norm_two, after(part_two, d_pre), TN)
        own_up = dp_scatter(part_up)

        x_in = after(part_up, x_saved)
        norm_one = (normed(x_in, mean_one, rstd_one) * wide(gain_one)).astype(lo)
        qkv = dot(norm_one, w_qkv_flat).astype(lo)
        d_norm_two = tp_scatter(part_two, part_up, qkv)
        hat_cut = normed(cut(h_saved), cut(mean_two), cut(rstd_two))
        d_mid = wide(cut(grad_y)) + norm_back(d_norm_two, hat_cut, cut(rstd_two), gain_two)
        d_mid_cut = d_mid.astype(lo)
        d_mid_lo = tp_gather(d_mid_cut, part_two)
        d_attn = dot(d_mid_lo, w_proj_flat, NT).astype(lo)
        own_down = after(d_attn, own_down).astype(lo)
        down_pieces = dp_ring.gather(own_down)
        attn_out, d_qkv = attention(qkv, after(own_down, d_attn), heads, head_dim)
        part_qkv = dot(norm_one, d_qkv, TN)
        own_qkv = dp_scatter(part_qkv)
        part_one = dot(after(part_qkv, d_qkv), w_qkv_flat, NT).astype(lo)
        part_proj = dot(after(part_one, attn_out), d_mid_lo, TN)
        own_proj = dp_scatter(part_proj)
        own_up = after(part_proj, own_up).astype(lo)
        up_pieces = dp_ring.gather(own_up)
        d_norm_one = tp_scatter(part_one, own_up, None)
        x_hat_cut = normed(cut(x_saved), cut(mean_one), cut(rstd_one))
        grad_x_cut = (d_mid + norm_back(d_norm_one, x_hat_cut, cut(rstd_one), gain_one)).astype(lo)
        own_qkv = own_qkv.astype(lo)
        grad_x = tp_gather(grad_x_cut, part_one, own_qkv)

        qkv_pieces = dp_ring.gather(own_qkv)
        late = lambda first, pieces: [(at, row, after(first, piece)) for at, row, piece in pieces]
        up_pieces = up_pieces[:-2] + late(own_qkv, up_pieces[-2:])
        own_proj = after((grad_x, qkv_pieces[:-2]), own_proj).astype(lo)
        proj_pieces = dp_ring.gather(own_proj)
        grad_down = dp_ring.placed(down_pieces, own_down.shape[0])
        grad_up = dp_ring.placed(up_pieces, own_up.shape[0])
        grad_qkv = dp_ring.placed(qkv_pieces, own_qkv.shape[0])
        grad_proj = dp_ring.placed(proj_pieces, own_proj.shape[0])
        return (grad_x, grad_qkv.reshape(w_qkv.shape), grad_proj.reshape(w_proj.shape), grad_up, grad_down)

    return jax.shard_map(local_step, mesh=mesh, in_specs=in_specs, out_specs=out_specs, check_vma=False)
```

```python
import functools
import math
import jax
import jax.numpy as jnp
from jax import lax
from jax.experimental import pallas as pl
from jax.experimental.pallas import tpu as pltpu
from jax.sharding import PartitionSpec as P

GELU_C = math.sqrt(2.0 / math.pi)
LOG2E = math.log2(math.e)
NT = (((1,), (1,)), ((), ()))
NN = (((1,), (0,)), ((), ()))
TN = (((0,), (0,)), ((), ()))


def dot(lhs, rhs, dims=NN):
    return lax.dot_general(lhs, rhs, dims, preferred_element_type=jnp.float32)


def normed(row_vals, row_mean, row_rstd):
    return (row_vals.astype(jnp.float32) - row_mean[:, None]) * row_rstd[:, None]


def norm_back(d_norm, x_hat, row_rstd, gain_vec):
    scaled = d_norm * gain_vec.astype(jnp.float32)
    scaled_mean = jnp.mean(scaled, axis=-1, keepdims=True)
    proj_mean = jnp.mean(scaled * x_hat, axis=-1, keepdims=True)
    return row_rstd[:, None] * (scaled - scaled_mean - x_hat * proj_mean)


def gelu_pair(pre_act):
    pre_wide = pre_act.astype(jnp.float32)
    tanh_val = jnp.tanh(GELU_C * (pre_wide + 0.044715 * pre_wide * pre_wide * pre_wide))
    gelu_val = 0.5 * pre_wide * (1.0 + tanh_val)
    gelu_slope = 0.5 * (1.0 + tanh_val) + 0.5 * pre_wide * (1.0 - tanh_val * tanh_val) * GELU_C * (1.0 + 0.134145 * pre_wide * pre_wide)
    return gelu_val, gelu_slope


def attn_kernel(head_dim, q_rows, q_ref, k_ref, v_ref, do_ref, o_ref, dqkv_ref, dk_acc, dv_acc):
    toks, lanes = q_ref.shape
    step = pl.program_id(0)
    per_block = lanes // head_dim
    group = step // per_block
    inner = lax.rem(step, per_block)
    width = dqkv_ref.shape[1] // 3
    scale = head_dim ** -0.5

    @pl.when(inner == 0)
    def _():
        dk_acc[...] = jnp.zeros_like(dk_acc)
        dv_acc[...] = jnp.zeros_like(dv_acc)
        o_ref[...] = jnp.zeros_like(o_ref)
        dqkv_ref[:, pl.ds(pl.multiple_of(group * lanes, lanes), lanes)] = jnp.zeros((toks, lanes), dqkv_ref.dtype)

    lane_ids = lax.broadcasted_iota(jnp.int32, (1, lanes), 1)
    mine = lane_ids // head_dim == inner
    zero = jnp.zeros((), jnp.bfloat16)
    k_own = jnp.where(mine, k_ref[...], zero)
    v_own = jnp.where(mine, v_ref[...], zero)
    k_t = k_own.T
    v_t = v_own.T
    q_cols = pl.ds(pl.multiple_of(group * lanes, lanes), lanes)
    for blk in range(toks // q_rows):
        rows = slice(blk * q_rows, (blk + 1) * q_rows)
        keys = (blk + 1) * q_rows
        q_blk = jnp.where(mine, q_ref[rows, :], zero)
        do_blk = jnp.where(mine, do_ref[rows, :], zero)
        s_t = dot(k_own[:keys], q_blk, NT)
        key_ids = lax.broadcasted_iota(jnp.int32, (q_rows, q_rows), 0)
        qry_ids = lax.broadcasted_iota(jnp.int32, (q_rows, q_rows), 1)
        s_diag = jnp.where(key_ids <= qry_ids, s_t[keys - q_rows:], -1e30)
        s_t = s_diag if blk == 0 else jnp.concatenate([s_t[:keys - q_rows], s_diag], axis=0)
        top = jnp.max(s_t, axis=0, keepdims=True)
        e_t = jnp.exp2((s_t - top) * (scale * LOG2E))
        p_t = e_t * (1.0 / jnp.sum(e_t, axis=0, keepdims=True))
        p_lo = p_t.astype(jnp.bfloat16)
        dp_t = dot(v_own[:keys], do_blk, NT)
        dv_acc[:keys] += dot(p_lo, do_blk)
        o_blk = dot(v_t[:, :keys], p_lo)
        o_ref[rows, :] += o_blk.T.astype(o_ref.dtype)
        prod = p_t * dp_t
        row_sum = jnp.sum(prod, axis=0, keepdims=True)
        ds_lo = (prod - p_t * row_sum).astype(jnp.bfloat16)
        dk_acc[:keys] += dot(ds_lo, q_blk)
        dq_blk = dot(k_t[:, :keys], ds_lo) * scale
        dqkv_ref[rows, q_cols] += dq_blk.T.astype(dqkv_ref.dtype)

    @pl.when(inner == per_block - 1)
    def _():
        dqkv_ref[:, pl.ds(pl.multiple_of(width + group * lanes, lanes), lanes)] = (dk_acc[...] * scale).astype(dqkv_ref.dtype)
        dqkv_ref[:, pl.ds(pl.multiple_of(2 * width + group * lanes, lanes), lanes)] = dv_acc[...].astype(dqkv_ref.dtype)


def attention(qkv, d_attn, heads, head_dim, q_rows=256):
    toks, width = d_attn.shape
    lanes = 128
    per_block = lanes // head_dim
    groups = width // lanes
    spec = lambda off: pl.BlockSpec((toks, lanes), lambda h: (0, off * groups + h // per_block))
    pairs = heads * toks * toks // 2
    return pl.pallas_call(
        functools.partial(attn_kernel, head_dim, q_rows),
        grid=(heads,),
        in_specs=[spec(0), spec(1), spec(2), spec(0)],
        out_specs=[spec(0), pl.BlockSpec((toks, 3 * width), lambda h: (0, 0))],
        out_shape=[jax.ShapeDtypeStruct((toks, width), jnp.bfloat16), jax.ShapeDtypeStruct((toks, 3 * width), jnp.bfloat16)],
        scratch_shapes=[pltpu.VMEM((toks, lanes), jnp.float32), pltpu.VMEM((toks, lanes), jnp.float32)],
        compiler_params=pltpu.CompilerParams(dimension_semantics=("arbitrary",), vmem_limit_bytes=48 * 2 ** 20),
        cost_estimate=pl.CostEstimate(flops=6 * 2 * 256 * pairs, bytes_accessed=8 * toks * width * 2, transcendentals=pairs),
        name="attn_fwd_bwd",
    )(qkv, qkv, qkv, d_attn)


def after(first, *later):
    out = lax.optimization_barrier((first,) + later)[1:]
    return out[0] if len(out) == 1 else out


def wide(arr):
    return arr.astype(jnp.float32)


def assemble_kernel(places, shape, *refs):
    n = len(places)
    pieces, out, held, in_sem, out_sem = refs[:n], refs[n], refs[n + 1:2 * n + 1], refs[2 * n + 1], refs[2 * n + 2]
    copies_in = [pltpu.make_async_copy(pieces[i], held[i], in_sem.at[i]) for i in range(n)]
    for copy in copies_in:
        copy.start()
    copies_out = []
    for i, place in enumerate(places):
        rows = pl.ds(pl.multiple_of(place(), 16), shape[i])
        copies_in[i].wait()
        copies_out.append(pltpu.make_async_copy(held[i], out.at[rows], out_sem.at[i]))
        copies_out[i].start()
    for copy in copies_out:
        copy.wait()


def assemble(placed):
    places, pieces = [p for p, _ in placed], [arr for _, arr in placed]
    n, cols, dtype = len(pieces), pieces[0].shape[1], pieces[0].dtype
    rows = sum(arr.shape[0] for arr in pieces)
    return pl.pallas_call(
        functools.partial(assemble_kernel, places, [arr.shape[0] for arr in pieces]),
        in_specs=[pl.BlockSpec(memory_space=pl.ANY)] * n,
        out_specs=pl.BlockSpec(memory_space=pl.ANY),
        out_shape=jax.ShapeDtypeStruct((rows, cols), dtype),
        scratch_shapes=[pltpu.VMEM(arr.shape, dtype) for arr in pieces] + [pltpu.SemaphoreType.DMA((n,)), pltpu.SemaphoreType.DMA((n,))],
        cost_estimate=pl.CostEstimate(flops=1000 * rows * 2, bytes_accessed=4 * rows * cols, transcendentals=0),
        name="assemble",
    )(*pieces)


class Ring:
    def __init__(self, axis, ways, lanes):
        self.axis, self.n, self.lanes = axis, ways // lanes, lanes
        hop = lambda d: [(i, ((i // lanes + d) % self.n) * lanes + i % lanes) for i in range(ways)]
        self.right, self.left = hop(1), hop(-1)

    def to(self, arr, pairs):
        return lax.ppermute(arr, self.axis, pairs)

    def at(self, d):
        return lax.rem(lax.axis_index(self.axis) // self.lanes + d + self.n, self.n)

    def gather(self, own, way=0):
        half = own.shape[0] // 2
        far = self.n // 2
        pieces = [(0, 0, own)]
        from_left = from_right = own
        for k in range(1, far):
            from_left, from_right = self.to(from_left, self.right), self.to(from_right, self.left)
            pieces += [(-k, 0, from_left), (k, 0, from_right)]
        if way:
            return pieces + [(far, 0, self.to(from_left, self.right) if way > 0 else self.to(from_right, self.left))]
        return pieces + [(far, 0, self.to(from_left[:half], self.right)), (far, half, self.to(from_right[half:], self.left))]

    def placed(self, pieces, rows):
        return assemble([(functools.partial(lambda offset, row: self.at(offset) * rows + row, offset, row), arr) for offset, row, arr in pieces])

    def scatter(self, blocks, filler):
        dtype = blocks.dtype
        half = blocks.shape[1] // 2
        blk = lambda d: lax.dynamic_index_in_dim(blocks, self.at(d), 0, keepdims=False)
        far = blk(self.n // 2)
        right, left = self.to(far[:half], self.right), self.to(far[half:], self.left)
        if filler is not None:
            right, left = after(filler, right, left)
        for k in range(self.n // 2 - 1, 0, -1):
            go_right, go_left = blk(k), blk(-k)
            if right.shape[0] == half:
                go_right = jnp.concatenate([(wide(go_right[:half]) + wide(right)).astype(dtype), go_right[half:]], 0)
                go_left = jnp.concatenate([go_left[:half], (wide(go_left[half:]) + wide(left)).astype(dtype)], 0)
            else:
                go_right = (wide(go_right) + wide(right)).astype(dtype)
                go_left = (wide(go_left) + wide(left)).astype(dtype)
            right, left = self.to(go_right, self.right), self.to(go_left, self.left)
        return wide(blk(0)) + wide(right) + wide(left)


def solution(mesh):
    row_spec = P(('pod', 'dp'), None)
    stat_spec = P(('pod', 'dp'))
    in_specs = (row_spec, row_spec, stat_spec, stat_spec, stat_spec, stat_spec, P(None), P(None), row_spec,
                P(None, None, 'tp', None), P('tp', None, None), P(None, 'tp'), P('tp', None))
    out_specs = (row_spec, P('pod', None, 'tp', None), P(('pod', 'tp'), None, None), P('pod', 'tp'), P(('pod', 'tp'), None))
    tp_ways, dp_ways = mesh.shape['tp'], mesh.shape['dp']
    cores = 2

    def local_step(x_saved, h_saved, mean_one, rstd_one, mean_two, rstd_two, gain_one, gain_two, grad_y, w_qkv, w_proj, w_up, w_down):
        toks, dim = x_saved.shape
        _, three, heads, head_dim = w_qkv.shape
        share = toks // tp_ways
        chips = tp_ways // cores
        tp_at = lax.axis_index('tp')
        start = tp_at * share
        cut = lambda arr: lax.dynamic_slice_in_dim(arr, start, share, 0)
        w_qkv_t = w_qkv.transpose(1, 2, 3, 0).reshape(three * heads * head_dim, dim)
        w_proj_flat = w_proj.reshape(heads * head_dim, dim)
        lo = jnp.bfloat16
        dp_ring = Ring('dp', dp_ways, 1)
        tp_ring = Ring('tp', tp_ways, cores)
        core = lax.rem(tp_at, cores)
        sibling = [(i, i ^ 1) for i in range(tp_ways)]

        def tp_scatter(part, first, second):
            by_core = part.reshape(chips, cores, share, dim)
            mine = lax.dynamic_index_in_dim(by_core, core, 1, keepdims=False)
            other = lax.dynamic_index_in_dim(by_core, 1 - core, 1, keepdims=False)
            other = after(first, lax.ppermute(other, 'tp', sibling))
            pair = (wide(mine) + wide(other)).astype(part.dtype)
            return tp_ring.scatter(pair, second)

        def tp_gather(own, first=None):
            placed = []
            for offset, row, piece in tp_ring.gather(own):
                if offset != 0 and first is not None:
                    piece = after(first, piece)
                at_core = lambda other, offset=offset, row=row: (tp_ring.at(offset) * cores + lax.rem(lax.axis_index('tp') + other, cores)) * share + row
                placed += [(functools.partial(at_core, 0), piece), (functools.partial(at_core, 1), lax.ppermute(piece, 'tp', sibling))]
            return assemble(placed)

        def dp_scatter(part):
            return lax.psum_scatter(part, 'dp', scatter_dimension=0, tiled=True)

        norm_two = (normed(h_saved, mean_two, rstd_two) * wide(gain_two)).astype(lo)
        pre_act = dot(norm_two, w_up).astype(lo)
        act_out = gelu_pair(pre_act)[0].astype(lo)
        part_down = dot(act_out, grad_y, TN)
        own_down = dp_scatter(part_down)
        pre_act, dy = after(part_down, pre_act, grad_y)
        d_pre = (dot(dy, w_down, NT) * gelu_pair(pre_act)[1]).astype(lo)
        part_two = dot(d_pre, w_up, NT).astype(lo)
        part_up = dot(norm_two, after(part_two, d_pre), TN)
        own_up = dp_scatter(part_up)

        x_in = after(part_up, x_saved)
        norm_one = (normed(x_in, mean_one, rstd_one) * wide(gain_one)).astype(lo)
        qkv = dot(norm_one, w_qkv_t, NT).astype(lo)
        d_norm_two = tp_scatter(part_two, part_up, qkv)
        hat_cut = normed(cut(h_saved), cut(mean_two), cut(rstd_two))
        d_mid = wide(cut(grad_y)) + norm_back(d_norm_two, hat_cut, cut(rstd_two), gain_two)
        d_mid_cut = d_mid.astype(lo)
        own_down = after(d_mid_cut, own_down).astype(lo)
        down_pieces = dp_ring.gather(own_down)
        d_mid_lo = tp_gather(d_mid_cut, own_down)
        d_attn = dot(d_mid_lo, w_proj_flat, NT).astype(lo)
        attn_out, d_qkv = attention(qkv, d_attn, heads, head_dim)
        part_qkv = dot(d_qkv, norm_one, TN)
        own_qkv = dp_scatter(part_qkv)
        part_one = dot(after(part_qkv, d_qkv), w_qkv_t).astype(lo)
        part_proj = dot(after(part_one, attn_out), d_mid_lo, TN)
        own_proj = dp_scatter(part_proj)
        own_up = after(part_proj, own_up).astype(lo)
        up_pieces = dp_ring.gather(own_up)
        d_norm_one = tp_scatter(part_one, own_up, None)
        x_hat_cut = normed(cut(x_saved), cut(mean_one), cut(rstd_one))
        grad_x_cut = (d_mid + norm_back(d_norm_one, x_hat_cut, cut(rstd_one), gain_one)).astype(lo)
        own_qkv = own_qkv.astype(lo)
        grad_x = tp_gather(grad_x_cut, own_qkv)

        qkv_pieces = dp_ring.gather(own_qkv)
        late = lambda first, pieces: [(at, row, after(first, piece)) for at, row, piece in pieces]
        up_pieces = up_pieces[:-2] + late(own_qkv, up_pieces[-2:])
        grad_down = dp_ring.placed(down_pieces, own_down.shape[0])
        grad_up = dp_ring.placed(up_pieces, own_up.shape[0])
        own_proj = after((grad_x, grad_down, grad_up), own_proj).astype(lo)
        proj_pieces = dp_ring.gather(own_proj, 1)
        grad_qkv = dp_ring.placed(qkv_pieces, own_qkv.shape[0])
        grad_proj = dp_ring.placed(proj_pieces, own_proj.shape[0])
        return (grad_x, grad_qkv.reshape(three, heads, head_dim, dim).transpose(3, 0, 1, 2), grad_proj.reshape(w_proj.shape), grad_up, grad_down)

    return jax.shard_map(local_step, mesh=mesh, in_specs=in_specs, out_specs=out_specs, check_vma=False)
```

```python
import functools
import math
import jax
import jax.numpy as jnp
from jax import lax
from jax.experimental import pallas as pl
from jax.experimental.pallas import tpu as pltpu
from jax.sharding import PartitionSpec as P

GELU_C = math.sqrt(2.0 / math.pi)
LOG2E = math.log2(math.e)
NT = (((1,), (1,)), ((), ()))
NN = (((1,), (0,)), ((), ()))
TN = (((0,), (0,)), ((), ()))


def dot(lhs, rhs, dims=NN):
    return lax.dot_general(lhs, rhs, dims, preferred_element_type=jnp.float32)


def normed(row_vals, row_mean, row_rstd):
    return (row_vals.astype(jnp.float32) - row_mean[:, None]) * row_rstd[:, None]


def norm_back(d_norm, x_hat, row_rstd, gain_vec):
    scaled = d_norm * gain_vec.astype(jnp.float32)
    scaled_mean = jnp.mean(scaled, axis=-1, keepdims=True)
    proj_mean = jnp.mean(scaled * x_hat, axis=-1, keepdims=True)
    return row_rstd[:, None] * (scaled - scaled_mean - x_hat * proj_mean)


def gelu_pair(pre_act):
    pre_wide = pre_act.astype(jnp.float32)
    tanh_val = jnp.tanh(GELU_C * (pre_wide + 0.044715 * pre_wide * pre_wide * pre_wide))
    gelu_val = 0.5 * pre_wide * (1.0 + tanh_val)
    gelu_slope = 0.5 * (1.0 + tanh_val) + 0.5 * pre_wide * (1.0 - tanh_val * tanh_val) * GELU_C * (1.0 + 0.134145 * pre_wide * pre_wide)
    return gelu_val, gelu_slope


def attn_kernel(head_dim, q_rows, q_ref, k_ref, v_ref, do_ref, o_ref, dqkv_ref, dk_acc, dv_acc):
    toks, lanes = q_ref.shape
    step = pl.program_id(0)
    per_block = lanes // head_dim
    group = step // per_block
    inner = lax.rem(step, per_block)
    width = dqkv_ref.shape[1] // 3
    scale = head_dim ** -0.5

    @pl.when(inner == 0)
    def _():
        dk_acc[...] = jnp.zeros_like(dk_acc)
        dv_acc[...] = jnp.zeros_like(dv_acc)
        o_ref[...] = jnp.zeros_like(o_ref)
        dqkv_ref[:, pl.ds(pl.multiple_of(group * lanes, lanes), lanes)] = jnp.zeros((toks, lanes), dqkv_ref.dtype)

    lane_ids = lax.broadcasted_iota(jnp.int32, (1, lanes), 1)
    mine = lane_ids // head_dim == inner
    zero = jnp.zeros((), jnp.bfloat16)
    k_own = jnp.where(mine, k_ref[...], zero)
    v_own = jnp.where(mine, v_ref[...], zero)
    k_t = k_own.T
    v_t = v_own.T
    q_cols = pl.ds(pl.multiple_of(group * lanes, lanes), lanes)
    for blk in range(toks // q_rows):
        rows = slice(blk * q_rows, (blk + 1) * q_rows)
        keys = (blk + 1) * q_rows
        q_blk = jnp.where(mine, q_ref[rows, :], zero)
        do_blk = jnp.where(mine, do_ref[rows, :], zero)
        s_t = dot(k_own[:keys], q_blk, NT)
        key_ids = lax.broadcasted_iota(jnp.int32, (q_rows, q_rows), 0)
        qry_ids = lax.broadcasted_iota(jnp.int32, (q_rows, q_rows), 1)
        s_diag = jnp.where(key_ids <= qry_ids, s_t[keys - q_rows:], -1e30)
        s_t = s_diag if blk == 0 else jnp.concatenate([s_t[:keys - q_rows], s_diag], axis=0)
        top = jnp.max(s_t, axis=0, keepdims=True)
        e_t = jnp.exp2((s_t - top) * (scale * LOG2E))
        p_t = e_t * (1.0 / jnp.sum(e_t, axis=0, keepdims=True))
        p_lo = p_t.astype(jnp.bfloat16)
        dp_t = dot(v_own[:keys], do_blk, NT)
        dv_acc[:keys] += dot(p_lo, do_blk)
        o_blk = dot(v_t[:, :keys], p_lo)
        o_ref[rows, :] += o_blk.T.astype(o_ref.dtype)
        prod = p_t * dp_t
        row_sum = jnp.sum(prod, axis=0, keepdims=True)
        ds_lo = (prod - p_t * row_sum).astype(jnp.bfloat16)
        dk_acc[:keys] += dot(ds_lo, q_blk)
        dq_blk = dot(k_t[:, :keys], ds_lo) * scale
        dqkv_ref[rows, q_cols] += dq_blk.T.astype(dqkv_ref.dtype)

    @pl.when(inner == per_block - 1)
    def _():
        dqkv_ref[:, pl.ds(pl.multiple_of(width + group * lanes, lanes), lanes)] = (dk_acc[...] * scale).astype(dqkv_ref.dtype)
        dqkv_ref[:, pl.ds(pl.multiple_of(2 * width + group * lanes, lanes), lanes)] = dv_acc[...].astype(dqkv_ref.dtype)


def attention(qkv, d_attn, heads, head_dim, q_rows=256):
    toks, width = d_attn.shape
    lanes = 128
    per_block = lanes // head_dim
    groups = width // lanes
    spec = lambda off: pl.BlockSpec((toks, lanes), lambda h: (0, off * groups + h // per_block))
    pairs = heads * toks * toks // 2
    return pl.pallas_call(
        functools.partial(attn_kernel, head_dim, q_rows),
        grid=(heads,),
        in_specs=[spec(0), spec(1), spec(2), spec(0)],
        out_specs=[spec(0), pl.BlockSpec((toks, 3 * width), lambda h: (0, 0))],
        out_shape=[jax.ShapeDtypeStruct((toks, width), jnp.bfloat16), jax.ShapeDtypeStruct((toks, 3 * width), jnp.bfloat16)],
        scratch_shapes=[pltpu.VMEM((toks, lanes), jnp.float32), pltpu.VMEM((toks, lanes), jnp.float32)],
        compiler_params=pltpu.CompilerParams(dimension_semantics=("arbitrary",), vmem_limit_bytes=48 * 2 ** 20),
        cost_estimate=pl.CostEstimate(flops=6 * 2 * 256 * pairs, bytes_accessed=8 * toks * width * 2, transcendentals=pairs),
        name="attn_fwd_bwd",
    )(qkv, qkv, qkv, d_attn)


def after(first, *later):
    out = lax.optimization_barrier((first,) + later)[1:]
    return out[0] if len(out) == 1 else out


def wide(arr):
    return arr.astype(jnp.float32)


def assemble_kernel(places, shape, *refs):
    n = len(places)
    pieces, out, held, in_sem, out_sem = refs[:n], refs[n], refs[n + 1:2 * n + 1], refs[2 * n + 1], refs[2 * n + 2]
    copies_in = [pltpu.make_async_copy(pieces[i], held[i], in_sem.at[i]) for i in range(n)]
    for copy in copies_in:
        copy.start()
    copies_out = []
    for i, place in enumerate(places):
        rows = pl.ds(pl.multiple_of(place(), 16), shape[i])
        copies_in[i].wait()
        copies_out.append(pltpu.make_async_copy(held[i], out.at[rows], out_sem.at[i]))
        copies_out[i].start()
    for copy in copies_out:
        copy.wait()


def assemble(placed):
    places, pieces = [p for p, _ in placed], [arr for _, arr in placed]
    n, cols, dtype = len(pieces), pieces[0].shape[1], pieces[0].dtype
    rows = sum(arr.shape[0] for arr in pieces)
    return pl.pallas_call(
        functools.partial(assemble_kernel, places, [arr.shape[0] for arr in pieces]),
        in_specs=[pl.BlockSpec(memory_space=pl.ANY)] * n,
        out_specs=pl.BlockSpec(memory_space=pl.ANY),
        out_shape=jax.ShapeDtypeStruct((rows, cols), dtype),
        scratch_shapes=[pltpu.VMEM(arr.shape, dtype) for arr in pieces] + [pltpu.SemaphoreType.DMA((n,)), pltpu.SemaphoreType.DMA((n,))],
        cost_estimate=pl.CostEstimate(flops=1000 * rows * 2, bytes_accessed=4 * rows * cols, transcendentals=0),
        name="assemble",
    )(*pieces)


class Ring:
    def __init__(self, axis, ways, lanes):
        self.axis, self.n, self.lanes = axis, ways // lanes, lanes
        hop = lambda d: [(i, ((i // lanes + d) % self.n) * lanes + i % lanes) for i in range(ways)]
        self.right, self.left = hop(1), hop(-1)

    def to(self, arr, pairs):
        return lax.ppermute(arr, self.axis, pairs)

    def at(self, d):
        return lax.rem(lax.axis_index(self.axis) // self.lanes + d + self.n, self.n)

    def gather(self, own, way=0):
        half = own.shape[0] // 2
        far = self.n // 2
        pieces = [(0, 0, own)]
        from_left = from_right = own
        for k in range(1, far):
            from_left, from_right = self.to(from_left, self.right), self.to(from_right, self.left)
            pieces += [(-k, 0, from_left), (k, 0, from_right)]
        if way:
            return pieces + [(far, 0, self.to(from_left, self.right) if way > 0 else self.to(from_right, self.left))]
        return pieces + [(far, 0, self.to(from_left[:half], self.right)), (far, half, self.to(from_right[half:], self.left))]

    def placed(self, pieces, rows):
        return assemble([(functools.partial(lambda offset, row: self.at(offset) * rows + row, offset, row), arr) for offset, row, arr in pieces])

    def scatter(self, blocks, filler, last=None):
        dtype = blocks.dtype
        half = blocks.shape[1] // 2
        blk = lambda d: lax.dynamic_index_in_dim(blocks, self.at(d), 0, keepdims=False)
        far = blk(self.n // 2)
        right, left = self.to(far[:half], self.right), self.to(far[half:], self.left)
        if filler is not None:
            right, left = after(filler, right, left)
        for k in range(self.n // 2 - 1, 0, -1):
            go_right, go_left = blk(k), blk(-k)
            if right.shape[0] == half:
                go_right = jnp.concatenate([(wide(go_right[:half]) + wide(right)).astype(dtype), go_right[half:]], 0)
                go_left = jnp.concatenate([go_left[:half], (wide(go_left[half:]) + wide(left)).astype(dtype)], 0)
            else:
                go_right = (wide(go_right) + wide(right)).astype(dtype)
                go_left = (wide(go_left) + wide(left)).astype(dtype)
            right, left = self.to(go_right, self.right), self.to(go_left, self.left)
        if last is not None:
            right, left = after(last, right, left)
        return wide(blk(0)) + wide(right) + wide(left)


def solution(mesh):
    row_spec = P(('pod', 'dp'), None)
    stat_spec = P(('pod', 'dp'))
    in_specs = (row_spec, row_spec, stat_spec, stat_spec, stat_spec, stat_spec, P(None), P(None), row_spec,
                P(None, None, 'tp', None), P('tp', None, None), P(None, 'tp'), P('tp', None))
    out_specs = (row_spec, P('pod', None, 'tp', None), P(('pod', 'tp'), None, None), P('pod', 'tp'), P(('pod', 'tp'), None))
    tp_ways, dp_ways = mesh.shape['tp'], mesh.shape['dp']
    cores = 2

    def local_step(x_saved, h_saved, mean_one, rstd_one, mean_two, rstd_two, gain_one, gain_two, grad_y, w_qkv, w_proj, w_up, w_down):
        toks, dim = x_saved.shape
        _, three, heads, head_dim = w_qkv.shape
        share = toks // tp_ways
        chips = tp_ways // cores
        tp_at = lax.axis_index('tp')
        start = tp_at * share
        cut = lambda arr: lax.dynamic_slice_in_dim(arr, start, share, 0)
        w_qkv_t = w_qkv.transpose(1, 2, 3, 0).reshape(three * heads * head_dim, dim)
        w_proj_flat = w_proj.reshape(heads * head_dim, dim)
        lo = jnp.bfloat16
        dp_ring = Ring('dp', dp_ways, 1)
        tp_ring = Ring('tp', tp_ways, cores)
        core = lax.rem(tp_at, cores)
        sibling = [(i, i ^ 1) for i in range(tp_ways)]

        def tp_scatter(part, first, second):
            by_core = part.reshape(chips, cores, share, dim)
            mine = lax.dynamic_index_in_dim(by_core, core, 1, keepdims=False)
            other = lax.dynamic_index_in_dim(by_core, 1 - core, 1, keepdims=False)
            other = after(first, lax.ppermute(other, 'tp', sibling))
            pair = (wide(mine) + wide(other)).astype(part.dtype)
            return tp_ring.scatter(pair, second)

        def tp_gather(own, first=None):
            placed = []
            for offset, row, piece in tp_ring.gather(own):
                if offset != 0 and first is not None:
                    piece = after(first, piece)
                at_core = lambda other, offset=offset, row=row: (tp_ring.at(offset) * cores + lax.rem(lax.axis_index('tp') + other, cores)) * share + row
                placed += [(functools.partial(at_core, 0), piece), (functools.partial(at_core, 1), lax.ppermute(piece, 'tp', sibling))]
            return assemble(placed)

        def dp_scatter(part):
            return lax.psum_scatter(part, 'dp', scatter_dimension=0, tiled=True)

        norm_two = (normed(h_saved, mean_two, rstd_two) * wide(gain_two)).astype(lo)
        pre_act = dot(norm_two, w_up).astype(lo)
        act_out = gelu_pair(pre_act)[0].astype(lo)
        part_down = dot(act_out, grad_y, TN)
        own_down = dp_scatter(part_down)
        pre_act, dy = after(part_down, pre_act, grad_y)
        d_pre = (dot(dy, w_down, NT) * gelu_pair(pre_act)[1]).astype(lo)
        part_two = dot(d_pre, w_up, NT).astype(lo)
        part_up = dot(norm_two, after(part_two, d_pre), TN)

        x_in = after(part_up, x_saved)
        norm_one = (normed(x_in, mean_one, rstd_one) * wide(gain_one)).astype(lo)
        qkv = dot(norm_one, w_qkv_t, NT).astype(lo)
        d_norm_two = tp_scatter(part_two, part_up, qkv)
        hat_cut = normed(cut(h_saved), cut(mean_two), cut(rstd_two))
        d_mid = wide(cut(grad_y)) + norm_back(d_norm_two, hat_cut, cut(rstd_two), gain_two)
        d_mid_cut = d_mid.astype(lo)
        up_blocks = part_up.reshape(dp_ways, dim // dp_ways, part_up.shape[1])
        own_down = after(d_mid_cut, own_down).astype(lo)
        down_pieces = dp_ring.gather(own_down)
        d_mid_lo = tp_gather(d_mid_cut, own_down)
        d_attn = dot(d_mid_lo, w_proj_flat, NT).astype(lo)
        attn_out, d_qkv = attention(qkv, d_attn, heads, head_dim)
        part_qkv = dot(d_qkv, norm_one, TN)
        own_qkv = dp_scatter(part_qkv)
        part_one = dot(after(part_qkv, d_qkv), w_qkv_t).astype(lo)
        part_proj = dot(after(part_one, attn_out), d_mid_lo, TN)
        own_proj = dp_scatter(part_proj)
        own_up = dp_ring.scatter(up_blocks, d_mid_cut, part_proj).astype(lo)
        up_pieces = dp_ring.gather(own_up)
        d_norm_one = tp_scatter(part_one, own_up, None)
        x_hat_cut = normed(cut(x_saved), cut(mean_one), cut(rstd_one))
        grad_x_cut = (d_mid + norm_back(d_norm_one, x_hat_cut, cut(rstd_one), gain_one)).astype(lo)
        own_qkv = own_qkv.astype(lo)
        grad_x = tp_gather(grad_x_cut, own_qkv)

        qkv_pieces = dp_ring.gather(own_qkv)
        late = lambda first, pieces: [(at, row, after(first, piece)) for at, row, piece in pieces]
        up_pieces = up_pieces[:-2] + late(own_qkv, up_pieces[-2:])
        grad_down = dp_ring.placed(down_pieces, own_down.shape[0])
        grad_up = dp_ring.placed(up_pieces, own_up.shape[0])
        own_proj = after((grad_x, grad_down, grad_up), own_proj).astype(lo)
        proj_pieces = dp_ring.gather(own_proj, 1)
        grad_qkv = dp_ring.placed(qkv_pieces, own_qkv.shape[0])
        grad_proj = dp_ring.placed(proj_pieces, own_proj.shape[0])
        return (grad_x, grad_qkv.reshape(three, heads, head_dim, dim).transpose(3, 0, 1, 2), grad_proj.reshape(w_proj.shape), grad_up, grad_down)

    return jax.shard_map(local_step, mesh=mesh, in_specs=in_specs, out_specs=out_specs, check_vma=False)
```
